32 devices in a mesh: batch: 2 (over x), row: 4 (over z), col: 4 (over y, core).
Axes of the slice: x: 2, y: 2, z: 4, core: 2. Of those that a mesh axis runs over, the one named last changes fastest.
Arguments:
- a_mat: bfloat16 [6144, 32768], P(('batch', 'row'), 'col'), parts along dimension 0
Outputs:
- output: bfloat16 [6144, 3072], P(('batch', 'row'), 'col'), parts along dimension 0
There are 2 independent parts. The reference program is written for one: setup_inputs(seed, part) draws one part's arguments, and reference() takes and returns one part's arrays. A program takes and returns all parts, laid end to end along the dimension named above; each array names one.
All inputs are finite; a program needn't handle non-finite values.
Results may differ from the reference program's by a relative error of at most 0.001.
Values are sent between devices in bfloat16 or wider.
A program may use at most 1 GiB of HBM per device.

```python
import jax
import jax.numpy as jnp
from jax import lax

N = 3072
BLOCK = 256
M_COLS = 32768
ROW_GROUPS = 4
COL_GROUPS = 4


def setup_inputs(seed: int = 0, part: int = 0) -> dict:
    base_key = jax.random.fold_in(jax.random.key(seed), part)
    values = jax.random.normal(base_key, (N, M_COLS), jnp.float32) * (M_COLS ** -0.25)
    return {"a_mat": values.astype(jnp.bfloat16)}


def global_index(size, groups):
    stored = jnp.arange(size)
    per_group = size // groups
    group_id = stored // per_group
    within = stored % per_group
    return ((within // BLOCK) * groups + group_id) * BLOCK + within % BLOCK


def reference(a_mat):
    blocks = N // BLOCK
    natural = a_mat.reshape(ROW_GROUPS, blocks // ROW_GROUPS, BLOCK, M_COLS).transpose(1, 0, 2, 3)
    col_order = natural.reshape(blocks // COL_GROUPS, COL_GROUPS, BLOCK, M_COLS).transpose(1, 0, 2, 3).reshape(N, M_COLS)
    col_trans = col_order.T
    row_index = global_index(N, ROW_GROUPS).reshape(blocks, BLOCK)
    col_index = global_index(N, COL_GROUPS)

    def one_block(block_item):
        row_blk, idx_blk = block_item
        product = jnp.dot(row_blk, col_trans, preferred_element_type=jnp.float32)
        return jnp.where(idx_blk[:, None] >= col_index[None, :], product, 0.0).astype(jnp.bfloat16)

    result = lax.map(one_block, (a_mat.reshape(blocks, BLOCK, M_COLS), row_index))
    return result.reshape(N, N)
```

```python
import jax
import jax.numpy as jnp
from jax import lax
from jax.experimental import pallas as pl
from jax.experimental.pallas import tpu as pltpu
from jax.sharding import PartitionSpec as P

BLOCK = 256
HALF = BLOCK // 2
MESH = pl.DeviceIdType.MESH
STAGES = ((0, BLOCK), (BLOCK, BLOCK), (2 * BLOCK, HALF), (2 * BLOCK + HALF, HALF))
D0, R1, D1, R2A, R2B, D2 = range(6)
DIAG_ROW = {D0: 0, D1: BLOCK, D2: 2 * BLOCK}
SPLIT_ROW = {R2A: 2 * BLOCK, R2B: 2 * BLOCK + HALF}
SELF_TILES = ((0, 0), (1, 0), (2, 0), (1, 1), (2, 1), (2, 2))


def product(left, right):
    return lax.dot_general(left, right, (((1,), (1,)), ((), ())), preferred_element_type=jnp.float32)


def kernel(a_ref, out_ref, panel, chunk, own_part, own_recv, part, core_in, y_in, z1_in, z2_in,
           a_send, a_recv, own_sem, chunk_sem, self_send, self_recv,
           core_send, core_recv, y_send, y_recv, z1_send, z1_recv, z2_send, z2_recv):
    z = lax.axis_index('row')
    col = lax.axis_index('col')
    core = lax.rem(col, 2)
    y = lax.div(col, 2)
    odd = lax.rem(z, 2)
    peers = (z + 1 - 2 * odd, lax.rem(z + 2, 4), 3 - z)
    sibling = {'col': col + 1 - 2 * core}
    y_peer = {'col': lax.rem(col + 2, 4)}
    width = panel.shape[2]
    deep = chunk.shape[2]
    kept = col
    given = lax.rem(col + 2, 4)

    barrier = pltpu.get_barrier_semaphore()
    for dev in (sibling, y_peer, {'row': peers[0]}, {'row': peers[1]}, {'row': peers[2]}):
        pl.semaphore_signal(barrier, inc=1, device_id=dev, device_id_type=MESH)
    pl.semaphore_wait(barrier, 5)

    def remote(src, dst, send, recv, dev):
        return pltpu.make_async_remote_copy(src_ref=src, dst_ref=dst, send_sem=send, recv_sem=recv,
                                            device_id=dev, device_id_type=MESH)

    def a_copy(stage, hop):
        first, count = STAGES[stage]
        peer = peers[hop]
        cols = pl.ds(pl.multiple_of(peer * width, 128), width)
        return remote(a_ref.at[pl.ds(first, count), cols], panel.at[z, pl.ds(first, count)],
                      a_send.at[stage, hop], a_recv.at[stage, hop], {'row': peer})

    def start_sends(order):
        for stage in range(len(STAGES)):
            for hop in order:
                a_copy(stage, hop).start()

    pl.when(core == 0)(lambda: start_sends((1, 2, 0)))
    pl.when(core == 1)(lambda: start_sends((0, 2, 1)))
    own_copy = pltpu.make_async_copy(a_ref.at[:, pl.ds(pl.multiple_of(z * width, 128), width)], panel.at[z], own_sem)
    own_copy.start()

    def chunk_copy(idx, slot):
        cols = pl.ds(pl.multiple_of(idx * deep, 128), deep)
        return pltpu.make_async_copy(a_ref.at[:, cols], chunk.at[slot], chunk_sem.at[slot])

    chunk_copy(0, 0).start()
    out_ref[...] = jnp.zeros_like(out_ref)
    own_part[...] = jnp.zeros_like(own_part)
    chunks = a_ref.shape[1] // deep

    def self_step(idx, carry):
        slot = lax.rem(idx, 2)

        @pl.when(idx + 1 < chunks)
        def _():
            chunk_copy(idx + 1, 1 - slot).start()

        chunk_copy(idx, slot).wait()
        for tile, (up, down) in enumerate(SELF_TILES):
            own_part[tile] += product(chunk[slot, pl.ds(up * BLOCK, BLOCK), :], chunk[slot, pl.ds(down * BLOCK, BLOCK), :])
        return carry

    lax.fori_loop(0, chunks, self_step, 0)
    self_core = remote(own_part, own_recv.at[0], self_send.at[0], self_recv.at[0], sibling)
    self_y = remote(own_part, own_recv.at[1], self_send.at[1], self_recv.at[1], y_peer)
    right_core = core == odd
    right_y = y == lax.div(z, 2)
    pl.when(jnp.logical_not(right_core))(lambda: self_core.start())

    def self_core_add():
        @pl.when(right_core)
        def _():
            self_core.wait_recv()
            own_part[...] += own_recv[0]
            pl.when(jnp.logical_not(right_y))(lambda: self_y.start())

    def self_y_add():
        @pl.when(col == z)
        def _():
            self_y.wait_recv()
            own_part[...] += own_recv[1]
            below = lax.broadcasted_iota(jnp.int32, (BLOCK, BLOCK), 0) >= lax.broadcasted_iota(jnp.int32, (BLOCK, BLOCK), 1)
            for tile, (up, down) in enumerate(SELF_TILES):
                vals = own_part[tile]
                if up == down:
                    vals = jnp.where(below, vals, 0.0)
                out_ref[pl.ds(up * BLOCK, BLOCK), pl.ds(down * BLOCK, BLOCK)] = vals.astype(out_ref.dtype)

    def if_present(flow, c, e, more, act):
        cond = more
        if flow in DIAG_ROW:
            here = c + e + 1 < 4
            cond = here if more is None else jnp.logical_and(more, here)
        if cond is None:
            act()
        else:
            pl.when(cond)(act)

    def core_copy(flow, c, e):
        pair = lax.div(c, 2)
        return remote(part.at[flow, c, e], core_in.at[flow, pair, e], core_send.at[flow, pair, e],
                      core_recv.at[flow, pair, e], sibling)

    def y_copy(flow, e):
        return remote(part.at[flow, given, e], y_in.at[flow, e], y_send.at[flow, e], y_recv.at[flow, e], y_peer)

    def z1_copy(flow, e, r):
        pair = lax.div(r, 2)
        return remote(part.at[flow, kept, e], z1_in.at[flow, pair], z1_send.at[flow, pair], z1_recv.at[flow, pair],
                      {'row': peers[0]})

    def z2_copy(flow, e):
        return remote(part.at[flow, kept, e], z2_in.at[flow], z2_send.at[flow], z2_recv.at[flow], {'row': peers[1]})

    def each(act):
        lax.fori_loop(0, 3, lambda e, carry: (act(e), carry)[1], 0)

    def wait_stage(stage):
        if stage == 0:
            own_copy.wait()
        for hop in range(3):
            a_copy(stage, hop).wait_recv()

    def compute(flow):
        def c_step(c, carry):
            def tile(e):
                r = lax.rem(c + e + 1, 4)

                def act():
                    if flow in DIAG_ROW:
                        rows = pl.ds(DIAG_ROW[flow], BLOCK)
                        part[flow, c, e] = product(panel[r, rows, :], panel[c, rows, :])
                    elif flow in SPLIT_ROW:
                        left = panel[r, pl.ds(SPLIT_ROW[flow], HALF), :]
                        for b in range(2):
                            part[flow, c, e, pl.ds(b * HALF, HALF), :] = product(left, panel[c, pl.ds(b * BLOCK, BLOCK), :])
                    else:
                        part[flow, c, e] = product(panel[r, pl.ds(BLOCK, BLOCK), :], panel[c, pl.ds(0, BLOCK), :])

                if_present(flow, c, e, None, act)

            each(tile)

            @pl.when(lax.rem(c, 2) != core)
            def _():
                each(lambda e: if_present(flow, c, e, None, lambda: core_copy(flow, c, e).start()))

            return carry

        lax.fori_loop(0, 4, c_step, 0)

    def core_add(flow):
        def add_in(c, e):
            core_copy(flow, c, e).wait_recv()
            part[flow, c, e] += core_in[flow, lax.div(c, 2), e]

        def pass_on(e):
            add_in(given, e)
            y_copy(flow, e).start()

        each(lambda e: if_present(flow, given, e, None, lambda: pass_on(e)))
        each(lambda e: if_present(flow, kept, e, None, lambda: add_in(kept, e)))

    def y_add(flow):
        def act(e):
            y_copy(flow, e).wait_recv()
            part[flow, kept, e] += y_in[flow, e]
            r = lax.rem(kept + e + 1, 4)
            pl.when(lax.rem(r, 2) != odd)(lambda: z1_copy(flow, e, r).start())

        each(lambda e: if_present(flow, kept, e, None, lambda: act(e)))

    def z1_add(flow):
        def act(e, r):
            z1_copy(flow, e, r).wait_recv()
            part[flow, kept, e] += z1_in[flow, lax.div(r, 2)]
            pl.when(r != z)(lambda: z2_copy(flow, e).start())

        def step(e):
            r = lax.rem(kept + e + 1, 4)
            if_present(flow, kept, e, lax.rem(r, 2) == odd, lambda: act(e, r))

        each(step)

    def z2_add(flow):
        def act(e):
            z2_copy(flow, e).wait_recv()
            vals = (part[flow, kept, e] + z2_in[flow]).astype(out_ref.dtype)
            if flow in DIAG_ROW:
                out_ref[pl.ds(DIAG_ROW[flow], BLOCK), pl.ds(DIAG_ROW[flow], BLOCK)] = vals
            elif flow in SPLIT_ROW:
                for b in range(2):
                    out_ref[pl.ds(SPLIT_ROW[flow], HALF), pl.ds(b * BLOCK, BLOCK)] = vals[b * HALF:(b + 1) * HALF]
            else:
                out_ref[pl.ds(BLOCK, BLOCK), pl.ds(0, BLOCK)] = vals

        each(lambda e: if_present(flow, kept, e, lax.rem(kept + e + 1, 4) == z, lambda: act(e)))

    def drain(flow):
        for pair in range(2):
            c = 1 - core + 2 * pair
            each(lambda e: if_present(flow, c, e, None, lambda: core_copy(flow, c, e).wait_send()))
        each(lambda e: if_present(flow, given, e, None, lambda: y_copy(flow, e).wait_send()))

        def step(e):
            r = lax.rem(kept + e + 1, 4)
            if_present(flow, kept, e, lax.rem(r, 2) != odd, lambda: z1_copy(flow, e, r).wait_send())
            if_present(flow, kept, e, r == lax.rem(z + 2, 4), lambda: z2_copy(flow, e).wait_send())

        each(step)

    wait_stage(0)
    compute(D0)
    self_core_add()
    core_add(D0)
    wait_stage(1)
    compute(R1)
    compute(D1)
    core_add(R1)
    core_add(D1)
    self_y_add()
    y_add(D0)
    wait_stage(2)
    compute(R2A)
    core_add(R2A)
    y_add(R1)
    y_add(D1)
    y_add(R2A)
    wait_stage(3)
    compute(R2B)
    core_add(R2B)
    compute(D2)
    core_add(D2)
    for flow in (D0, R1, D1, R2A):
        z1_add(flow)
    y_add(R2B)
    y_add(D2)
    z1_add(R2B)
    z1_add(D2)
    for flow in range(6):
        z2_add(flow)

    for stage in range(len(STAGES)):
        for hop in range(3):
            a_copy(stage, hop).wait_send()
    pl.when(jnp.logical_not(right_core))(lambda: self_core.wait_send())
    pl.when(jnp.logical_and(right_core, jnp.logical_not(right_y)))(lambda: self_y.wait_send())
    for flow in range(6):
        drain(flow)


def solution(mesh):
    def local_fn(a_local):
        local_rows, m_local = a_local.shape
        width = m_local // 4
        deep = min(1024, m_local)
        tile = (BLOCK, BLOCK)
        dma = pltpu.SemaphoreType.DMA
        return pl.pallas_call(
            kernel,
            out_shape=jax.ShapeDtypeStruct((local_rows, local_rows), jnp.bfloat16),
            in_specs=[pl.BlockSpec(memory_space=pl.ANY)],
            out_specs=pl.BlockSpec(memory_space=pltpu.VMEM),
            scratch_shapes=[
                pltpu.VMEM((4, local_rows, width), jnp.bfloat16),
                pltpu.VMEM((2, local_rows, deep), jnp.bfloat16),
                pltpu.VMEM((6,) + tile, jnp.float32),
                pltpu.VMEM((2, 6) + tile, jnp.float32),
                pltpu.VMEM((6, 4, 3) + tile, jnp.float32),
                pltpu.VMEM((6, 2, 3) + tile, jnp.float32),
                pltpu.VMEM((6, 3) + tile, jnp.float32),
                pltpu.VMEM((6, 2) + tile, jnp.float32),
                pltpu.VMEM((6,) + tile, jnp.float32),
                dma((4, 3)), dma((4, 3)), dma, dma((2,)), dma((2,)), dma((2,)),
                dma((6, 2, 3)), dma((6, 2, 3)), dma((6, 3)), dma((6, 3)),
                dma((6, 2)), dma((6, 2)), dma((6,)), dma((6,)),
            ],
            compiler_params=pltpu.CompilerParams(collective_id=0, has_side_effects=True, vmem_limit_bytes=67043328),
            name='triangle',
        )(a_local)

    part_spec = P(('batch', 'row'), 'col')
    return jax.shard_map(local_fn, mesh=mesh, in_specs=(part_spec,), out_specs=part_spec, check_vma=False)
```

```python
import jax
import jax.numpy as jnp
from jax import lax
from jax.experimental import pallas as pl
from jax.experimental.pallas import tpu as pltpu
from jax.sharding import PartitionSpec as P

BLOCK = 256
MESH = pl.DeviceIdType.MESH
STAGES = ((0, 256), (256, 256), (512, 128), (640, 64), (704, 64))
FIRST_STAGES = 3
FLOWS = 7
D0, R1, D1, R2A, R2B, R2C, D2 = range(FLOWS)
DIAG_ROW = {D0: 0, D1: BLOCK, D2: 2 * BLOCK}
SPLIT_ROW = {R2A: (512, 128), R2B: (640, 64), R2C: (704, 64)}
PLACE = {D0: (0, 0, 256), R1: (1, 0, 256), D1: (2, 0, 256), R2A: (3, 0, 256), R2B: (4, 0, 128), R2C: (4, 128, 128), D2: (5, 0, 256)}
SELF_TILES = ((0, 0), (1, 0), (2, 0), (1, 1), (2, 1), (2, 2))


def product(left, right):
    return lax.dot_general(left, right, (((1,), (1,)), ((), ())), preferred_element_type=jnp.float32)


def kernel(a_ref, out_ref, panel, chunk, own_part, own_recv, part, core_in, y_in, z1_in, z2_in, d_z1_in, d_z2_in,
           a_send, a_recv, own_sem, chunk_sem, self_send, self_recv,
           core_send, core_recv, y_send, y_recv, z1_send, z1_recv, z2_send, z2_recv,
           d_z1_send, d_z1_recv, d_z2_send, d_z2_recv):
    z = lax.axis_index('row')
    col = lax.axis_index('col')
    core = lax.rem(col, 2)
    y = lax.div(col, 2)
    odd = lax.rem(z, 2)
    peers = (z + 1 - 2 * odd, lax.rem(z + 2, 4), 3 - z)
    sibling = {'col': col + 1 - 2 * core}
    y_peer = {'col': lax.rem(col + 2, 4)}
    width = panel.shape[2]
    deep = chunk.shape[2]
    kept = col
    given = lax.rem(col + 2, 4)

    barrier = pltpu.get_barrier_semaphore()
    for dev in (sibling, y_peer, {'row': peers[0]}, {'row': peers[1]}, {'row': peers[2]}):
        pl.semaphore_signal(barrier, inc=1, device_id=dev, device_id_type=MESH)
    pl.semaphore_wait(barrier, 5)

    def remote(src, dst, send, recv, dev):
        return pltpu.make_async_remote_copy(src_ref=src, dst_ref=dst, send_sem=send, recv_sem=recv,
                                            device_id=dev, device_id_type=MESH)

    def a_copy(stage, hop):
        first, count = STAGES[stage]
        peer = peers[hop]
        cols = pl.ds(pl.multiple_of(peer * width, 128), width)
        return remote(a_ref.at[pl.ds(first, count), cols], panel.at[z, pl.ds(first, count)],
                      a_send.at[stage, hop], a_recv.at[stage, hop], {'row': peer})

    def start_sends(stages):
        def in_order(order):
            for stage in stages:
                for hop in order:
                    a_copy(stage, hop).start()

        pl.when(core == 0)(lambda: in_order((1, 2, 0)))
        pl.when(core == 1)(lambda: in_order((0, 2, 1)))

    start_sends(range(FIRST_STAGES))
    own_copy = pltpu.make_async_copy(a_ref.at[:, pl.ds(pl.multiple_of(z * width, 128), width)], panel.at[z], own_sem)
    own_copy.start()

    def chunk_copy(idx, slot):
        cols = pl.ds(pl.multiple_of(idx * deep, 128), deep)
        return pltpu.make_async_copy(a_ref.at[:, cols], chunk.at[slot], chunk_sem.at[slot])

    chunk_copy(0, 0).start()
    out_ref[...] = jnp.zeros_like(out_ref)
    own_part[...] = jnp.zeros_like(own_part)
    chunks = a_ref.shape[1] // deep

    def self_step(idx, carry):
        slot = lax.rem(idx, 2)

        @pl.when(idx + 1 < chunks)
        def _():
            chunk_copy(idx + 1, 1 - slot).start()

        chunk_copy(idx, slot).wait()
        for tile, (up, down) in enumerate(SELF_TILES):
            own_part[tile] += product(chunk[slot, pl.ds(up * BLOCK, BLOCK), :], chunk[slot, pl.ds(down * BLOCK, BLOCK), :])
        return carry

    lax.fori_loop(0, chunks, self_step, 0)
    self_core = remote(own_part, own_recv.at[0], self_send.at[0], self_recv.at[0], sibling)
    self_y = remote(own_part, own_recv.at[1], self_send.at[1], self_recv.at[1], y_peer)
    right_core = core == odd
    right_y = y == lax.div(z, 2)
    pl.when(jnp.logical_not(right_core))(lambda: self_core.start())

    def self_core_add():
        @pl.when(right_core)
        def _():
            self_core.wait_recv()
            own_part[...] += own_recv[0]
            pl.when(jnp.logical_not(right_y))(lambda: self_y.start())

    def self_y_add():
        @pl.when(col == z)
        def _():
            self_y.wait_recv()
            own_part[...] += own_recv[1]
            below = lax.broadcasted_iota(jnp.int32, (BLOCK, BLOCK), 0) >= lax.broadcasted_iota(jnp.int32, (BLOCK, BLOCK), 1)
            for tile, (up, down) in enumerate(SELF_TILES):
                vals = own_part[tile]
                if up == down:
                    vals = jnp.where(below, vals, 0.0)
                out_ref[pl.ds(up * BLOCK, BLOCK), pl.ds(down * BLOCK, BLOCK)] = vals.astype(out_ref.dtype)

    def if_present(flow, c, e, more, act):
        cond = more
        if flow in DIAG_ROW:
            here = c + e + 1 < 4
            cond = here if more is None else jnp.logical_and(more, here)
        if cond is None:
            act()
        else:
            pl.when(cond)(act)

    def view(ref, flow, *idx):
        slot, first, count = PLACE[flow]
        return ref.at[(slot,) + idx + (pl.ds(first, count),)]

    def core_copy(flow, c, e):
        pair = lax.div(c, 2)
        return remote(view(part, flow, c, e), view(core_in, flow, pair, e), core_send.at[flow, pair, e],
                      core_recv.at[flow, pair, e], sibling)

    def y_copy(flow, e):
        return remote(view(part, flow, given, e), view(y_in, flow, e), y_send.at[flow, e], y_recv.at[flow, e], y_peer)

    def z1_copy(flow, e, r):
        pair = lax.div(r, 2)
        return remote(view(part, flow, kept, e), view(z1_in, flow, pair), z1_send.at[flow, pair], z1_recv.at[flow, pair],
                      {'row': peers[0]})

    def z2_copy(flow, e):
        return remote(view(part, flow, kept, e), view(z2_in, flow), z2_send.at[flow], z2_recv.at[flow], {'row': peers[1]})

    def each(act):
        lax.fori_loop(0, 3, lambda e, carry: (act(e), carry)[1], 0)

    def wait_stage(stage):
        if stage == 0:
            own_copy.wait()
        for hop in range(3):
            a_copy(stage, hop).wait_recv()

    def compute(flow):
        slot, first, _ = PLACE[flow]

        def c_step(c, carry):
            def tile(e):
                r = lax.rem(c + e + 1, 4)

                def act():
                    if flow in DIAG_ROW:
                        rows = pl.ds(DIAG_ROW[flow], BLOCK)
                        part[slot, c, e] = product(panel[r, rows, :], panel[c, rows, :])
                    elif flow in SPLIT_ROW:
                        row, count = SPLIT_ROW[flow]
                        left = panel[r, pl.ds(row, count), :]
                        for b in range(2):
                            part[slot, c, e, pl.ds(first + b * count, count), :] = product(left, panel[c, pl.ds(b * BLOCK, BLOCK), :])
                    else:
                        part[slot, c, e] = product(panel[r, pl.ds(BLOCK, BLOCK), :], panel[c, pl.ds(0, BLOCK), :])

                if_present(flow, c, e, None, act)

            each(tile)

            @pl.when(lax.rem(c, 2) != core)
            def _():
                each(lambda e: if_present(flow, c, e, None, lambda: core_copy(flow, c, e).start()))

            return carry

        lax.fori_loop(0, 4, c_step, 0)

    def core_add(flow):
        def add_in(c, e):
            core_copy(flow, c, e).wait_recv()
            view(part, flow, c, e)[...] += view(core_in, flow, lax.div(c, 2), e)[...]

        def pass_on(e):
            add_in(given, e)
            y_copy(flow, e).start()

        if flow == D2:
            each_d(lambda pair, c, e, r: (add_in(c, e), pl.when(lax.rem(r, 2) != odd)(lambda: d_z1_copy(pair, c, e, r).start())))
            return
        each(lambda e: if_present(flow, given, e, None, lambda: pass_on(e)))
        each(lambda e: if_present(flow, kept, e, None, lambda: add_in(kept, e)))

    def y_add(flow):
        def act(e):
            y_copy(flow, e).wait_recv()
            view(part, flow, kept, e)[...] += view(y_in, flow, e)[...]
            r = lax.rem(kept + e + 1, 4)
            pl.when(lax.rem(r, 2) != odd)(lambda: z1_copy(flow, e, r).start())

        each(lambda e: if_present(flow, kept, e, None, lambda: act(e)))

    def z1_add(flow):
        def act(e, r):
            z1_copy(flow, e, r).wait_recv()
            view(part, flow, kept, e)[...] += view(z1_in, flow, lax.div(r, 2))[...]
            pl.when(r != z)(lambda: z2_copy(flow, e).start())

        def step(e):
            r = lax.rem(kept + e + 1, 4)
            if_present(flow, kept, e, lax.rem(r, 2) == odd, lambda: act(e, r))

        each(step)

    def z2_add(flow):
        def act(e):
            z2_copy(flow, e).wait_recv()
            vals = (view(part, flow, kept, e)[...] + view(z2_in, flow)[...]).astype(out_ref.dtype)
            if flow in DIAG_ROW:
                out_ref[pl.ds(DIAG_ROW[flow], BLOCK), pl.ds(DIAG_ROW[flow], BLOCK)] = vals
            elif flow in SPLIT_ROW:
                row, count = SPLIT_ROW[flow]
                for b in range(2):
                    out_ref[pl.ds(row, count), pl.ds(b * BLOCK, BLOCK)] = vals[b * count:(b + 1) * count]
            else:
                out_ref[pl.ds(BLOCK, BLOCK), pl.ds(0, BLOCK)] = vals

        each(lambda e: if_present(flow, kept, e, lax.rem(kept + e + 1, 4) == z, lambda: act(e)))

    def each_d(act):
        for pair in range(2):
            c = core + 2 * pair
            each(lambda e: pl.when(c + e + 1 < 4)(lambda: (act(pair, c, e, c + e + 1), None)[1]))

    def d_z1_copy(pair, c, e, r):
        half = lax.div(r, 2)
        return remote(part.at[5, c, e], d_z1_in.at[pair, half], d_z1_send.at[pair, half], d_z1_recv.at[pair, half],
                      {'row': peers[0]})

    def d_z2_copy(pair, c, e):
        return remote(part.at[5, c, e], d_z2_in.at[pair], d_z2_send.at[pair], d_z2_recv.at[pair], {'row': peers[1]})

    def d_y_copy(c, e):
        return remote(part.at[5, c, e], y_in.at[5, 0], y_send.at[D2, 0], y_recv.at[D2, 0], y_peer)

    def d_z1_add():
        def act(pair, c, e, r):
            @pl.when(lax.rem(r, 2) == odd)
            def _():
                d_z1_copy(pair, c, e, r).wait_recv()
                part[5, c, e] += d_z1_in[pair, lax.div(r, 2)]
                pl.when(r != z)(lambda: d_z2_copy(pair, c, e).start())

        each_d(act)

    def d_z2_add():
        def act(pair, c, e, r):
            @pl.when(r == z)
            def _():
                d_z2_copy(pair, c, e).wait_recv()
                part[5, c, e] += d_z2_in[pair]
                pl.when(y != pair)(lambda: d_y_copy(c, e).start())

        each_d(act)

    def d_y_add():
        def act(pair, c, e, r):
            @pl.when(jnp.logical_and(r == z, y == pair))
            def _():
                d_y_copy(c, e).wait_recv()
                rows = pl.ds(DIAG_ROW[D2], BLOCK)
                out_ref[rows, rows] = (part[5, c, e] + y_in[5, 0]).astype(out_ref.dtype)

        each_d(act)

    def d_drain():
        def act(pair, c, e, r):
            pl.when(lax.rem(r, 2) != odd)(lambda: d_z1_copy(pair, c, e, r).wait_send())
            pl.when(r == lax.rem(z + 2, 4))(lambda: d_z2_copy(pair, c, e).wait_send())
            pl.when(jnp.logical_and(r == z, y != pair))(lambda: d_y_copy(c, e).wait_send())

        each_d(act)

    def drain(flow):
        for pair in range(2):
            c = 1 - core + 2 * pair
            each(lambda e: if_present(flow, c, e, None, lambda: core_copy(flow, c, e).wait_send()))
        if flow == D2:
            d_drain()
            return
        each(lambda e: if_present(flow, given, e, None, lambda: y_copy(flow, e).wait_send()))

        def step(e):
            r = lax.rem(kept + e + 1, 4)
            if_present(flow, kept, e, lax.rem(r, 2) != odd, lambda: z1_copy(flow, e, r).wait_send())
            if_present(flow, kept, e, r == lax.rem(z + 2, 4), lambda: z2_copy(flow, e).wait_send())

        each(step)

    wait_stage(0)
    compute(D0)
    self_core_add()
    core_add(D0)
    wait_stage(1)
    compute(R1)
    core_add(R1)
    compute(D1)
    core_add(D1)
    self_y_add()
    y_add(D0)
    y_add(R1)
    start_sends(range(FIRST_STAGES, len(STAGES)))
    y_add(D1)
    wait_stage(2)
    compute(R2A)
    core_add(R2A)
    z1_add(D0)
    z1_add(R1)
    y_add(R2A)
    wait_stage(3)
    compute(R2B)
    core_add(R2B)
    y_add(R2B)
    wait_stage(4)
    compute(D2)
    compute(R2C)
    core_add(D2)
    core_add(R2C)
    z1_add(D1)
    z1_add(R2A)
    z1_add(R2B)
    d_z1_add()
    y_add(R2C)
    z2_add(D0)
    z2_add(R1)
    d_z2_add()
    z1_add(R2C)
    z2_add(D1)
    z2_add(R2A)
    z2_add(R2B)
    d_y_add()
    z2_add(R2C)

    for stage in range(len(STAGES)):
        for hop in range(3):
            a_copy(stage, hop).wait_send()
    pl.when(jnp.logical_not(right_core))(lambda: self_core.wait_send())
    pl.when(jnp.logical_and(right_core, jnp.logical_not(right_y)))(lambda: self_y.wait_send())
    for flow in range(FLOWS):
        drain(flow)


def solution(mesh):
    def local_fn(a_local):
        local_rows, m_local = a_local.shape
        width = m_local // 4
        deep = min(1024, m_local)
        tile = (BLOCK, BLOCK)
        dma = pltpu.SemaphoreType.DMA
        return pl.pallas_call(
            kernel,
            out_shape=jax.ShapeDtypeStruct((local_rows, local_rows), jnp.bfloat16),
            in_specs=[pl.BlockSpec(memory_space=pl.ANY)],
            out_specs=pl.BlockSpec(memory_space=pltpu.VMEM),
            scratch_shapes=[
                pltpu.VMEM((4, local_rows, width), jnp.bfloat16),
                pltpu.VMEM((2, local_rows, deep), jnp.bfloat16),
                pltpu.VMEM((6,) + tile, jnp.float32),
                pltpu.VMEM((2, 6) + tile, jnp.float32),
                pltpu.VMEM((6, 4, 3) + tile, jnp.float32),
                pltpu.VMEM((6, 2, 3) + tile, jnp.float32),
                pltpu.VMEM((6, 3) + tile, jnp.float32),
                pltpu.VMEM((5, 2) + tile, jnp.float32),
                pltpu.VMEM((5,) + tile, jnp.float32),
                pltpu.VMEM((2, 2) + tile, jnp.float32),
                pltpu.VMEM((2,) + tile, jnp.float32),
                dma((len(STAGES), 3)), dma((len(STAGES), 3)), dma, dma((2,)), dma((2,)), dma((2,)),
                dma((FLOWS, 2, 3)), dma((FLOWS, 2, 3)), dma((FLOWS, 3)), dma((FLOWS, 3)),
                dma((FLOWS, 2)), dma((FLOWS, 2)), dma((FLOWS,)), dma((FLOWS,)),
                dma((2, 2)), dma((2, 2)), dma((2,)), dma((2,)),
            ],
            compiler_params=pltpu.CompilerParams(collective_id=0, has_side_effects=True, vmem_limit_bytes=67043328),
            name='triangle',
        )(a_local)

    part_spec = P(('batch', 'row'), 'col')
    return jax.shard_map(local_fn, mesh=mesh, in_specs=(part_spec,), out_specs=part_spec, check_vma=False)
```

```python
import jax
import jax.numpy as jnp
from jax import lax
from jax.experimental import pallas as pl
from jax.experimental.pallas import tpu as pltpu
from jax.sharding import PartitionSpec as P

BLOCK = 256
MESH = pl.DeviceIdType.MESH
STAGES = ((0, 256), (256, 256), (512, 128), (640, 64), (704, 64))
FIRST_STAGES = 3
FLOWS = 7
D0, R1, D1, R2A, R2B, R2C, D2 = range(FLOWS)
DIAG_ROW = {D0: 0, D1: BLOCK, D2: 2 * BLOCK}
SPLIT_ROW = {R2A: (512, 128), R2B: (640, 64), R2C: (704, 64)}
PLACE = {D0: (0, 0, 256), R1: (1, 0, 256), D1: (2, 0, 256), R2A: (3, 0, 256), R2B: (4, 0, 128), R2C: (4, 128, 128), D2: (5, 0, 256)}
SELF_TILES = ((0, 0), (1, 0), (2, 0), (1, 1), (2, 1), (2, 2))


def product(left, right):
    return lax.dot_general(left, right, (((1,), (1,)), ((), ())), preferred_element_type=jnp.float32)


def kernel(a_ref, out_ref, panel, chunk, own_part, own_recv, part, core_in, y_in, z1_in, z2_in, d_z1_in, d_z2_in,
           a_send, a_recv, own_sem, chunk_sem, self_send, self_recv,
           core_send, core_recv, y_send, y_recv, z1_send, z1_recv, z2_send, z2_recv,
           d_z1_send, d_z1_recv, d_z2_send, d_z2_recv):
    z = lax.axis_index('row')
    col = lax.axis_index('col')
    core = lax.rem(col, 2)
    y = lax.div(col, 2)
    odd = lax.rem(z, 2)
    peers = (z + 1 - 2 * odd, lax.rem(z + 2, 4), 3 - z)
    sibling = {'col': col + 1 - 2 * core}
    y_peer = {'col': lax.rem(col + 2, 4)}
    width = panel.shape[2]
    deep = chunk.shape[2]
    kept = col
    given = lax.rem(col + 2, 4)

    barrier = pltpu.get_barrier_semaphore()
    for dev in (sibling, y_peer, {'row': peers[0]}, {'row': peers[1]}, {'row': peers[2]}):
        pl.semaphore_signal(barrier, inc=1, device_id=dev, device_id_type=MESH)
    pl.semaphore_wait(barrier, 5)

    def remote(src, dst, send, recv, dev):
        return pltpu.make_async_remote_copy(src_ref=src, dst_ref=dst, send_sem=send, recv_sem=recv,
                                            device_id=dev, device_id_type=MESH)

    def a_copy(stage, hop):
        first, count = STAGES[stage]
        peer = peers[hop]
        cols = pl.ds(pl.multiple_of(peer * width, 128), width)
        return remote(a_ref.at[pl.ds(first, count), cols], panel.at[z, pl.ds(first, count)],
                      a_send.at[stage, hop], a_recv.at[stage, hop], {'row': peer})

    inner = jnp.logical_or(z == 1, z == 2)
    outer = jnp.logical_not(inner)
    every = range(len(STAGES))

    def start_pairs(stages, one, two):
        def in_order(order):
            for stage in stages:
                for hop in order:
                    a_copy(stage, hop).start()

        pl.when(core == 0)(lambda: in_order((one, two)))
        pl.when(core == 1)(lambda: in_order((two, one)))

    @pl.when(inner)
    def _():
        for stage in every:
            a_copy(stage, 0).start()

    @pl.when(outer)
    def _():
        for stage in every:
            a_copy(stage, 1).start()
        start_pairs(every[:FIRST_STAGES], 2, 0)

    own_copy = pltpu.make_async_copy(a_ref.at[:, pl.ds(pl.multiple_of(z * width, 128), width)], panel.at[z], own_sem)
    own_copy.start()

    def chunk_copy(idx, slot):
        cols = pl.ds(pl.multiple_of(idx * deep, 128), deep)
        return pltpu.make_async_copy(a_ref.at[:, cols], chunk.at[slot], chunk_sem.at[slot])

    chunk_copy(0, 0).start()
    out_ref[...] = jnp.zeros_like(out_ref)
    own_part[...] = jnp.zeros_like(own_part)
    chunks = a_ref.shape[1] // deep

    def self_step(idx, carry):
        slot = lax.rem(idx, 2)

        @pl.when(idx + 1 < chunks)
        def _():
            chunk_copy(idx + 1, 1 - slot).start()

        chunk_copy(idx, slot).wait()
        for tile, (up, down) in enumerate(SELF_TILES):
            own_part[tile] += product(chunk[slot, pl.ds(up * BLOCK, BLOCK), :], chunk[slot, pl.ds(down * BLOCK, BLOCK), :])
        return carry

    lax.fori_loop(0, chunks, self_step, 0)
    self_core = remote(own_part, own_recv.at[0], self_send.at[0], self_recv.at[0], sibling)
    self_y = remote(own_part, own_recv.at[1], self_send.at[1], self_recv.at[1], y_peer)
    right_core = core == odd
    right_y = y == lax.div(z, 2)
    pl.when(jnp.logical_not(right_core))(lambda: self_core.start())

    @pl.when(inner)
    def _():
        for stage in every:
            a_copy(stage, 0).wait_send()
        start_pairs(every, 2, 1)

    def self_core_add():
        @pl.when(right_core)
        def _():
            self_core.wait_recv()
            own_part[...] += own_recv[0]
            pl.when(jnp.logical_not(right_y))(lambda: self_y.start())

    def self_y_add():
        @pl.when(col == z)
        def _():
            self_y.wait_recv()
            own_part[...] += own_recv[1]
            below = lax.broadcasted_iota(jnp.int32, (BLOCK, BLOCK), 0) >= lax.broadcasted_iota(jnp.int32, (BLOCK, BLOCK), 1)
            for tile, (up, down) in enumerate(SELF_TILES):
                vals = own_part[tile]
                if up == down:
                    vals = jnp.where(below, vals, 0.0)
                out_ref[pl.ds(up * BLOCK, BLOCK), pl.ds(down * BLOCK, BLOCK)] = vals.astype(out_ref.dtype)

    def if_present(flow, c, e, more, act):
        cond = more
        if flow in DIAG_ROW:
            here = c + e + 1 < 4
            cond = here if more is None else jnp.logical_and(more, here)
        if cond is None:
            act()
        else:
            pl.when(cond)(act)

    def view(ref, flow, *idx):
        slot, first, count = PLACE[flow]
        return ref.at[(slot,) + idx + (pl.ds(first, count),)]

    def core_copy(flow, c, e):
        pair = lax.div(c, 2)
        return remote(view(part, flow, c, e), view(core_in, flow, pair, e), core_send.at[flow, pair, e],
                      core_recv.at[flow, pair, e], sibling)

    def y_copy(flow, e):
        return remote(view(part, flow, given, e), view(y_in, flow, e), y_send.at[flow, e], y_recv.at[flow, e], y_peer)

    def z1_copy(flow, e, r):
        pair = lax.div(r, 2)
        return remote(view(part, flow, kept, e), view(z1_in, flow, pair), z1_send.at[flow, pair], z1_recv.at[flow, pair],
                      {'row': peers[0]})

    def z2_copy(flow, e):
        return remote(view(part, flow, kept, e), view(z2_in, flow), z2_send.at[flow], z2_recv.at[flow], {'row': peers[1]})

    def each(act):
        lax.fori_loop(0, 3, lambda e, carry: (act(e), carry)[1], 0)

    def wait_stage(stage):
        if stage == 0:
            own_copy.wait()
        for hop in range(3):
            a_copy(stage, hop).wait_recv()

    def compute(flow):
        slot, first, _ = PLACE[flow]

        def c_step(c, carry):
            def tile(e):
                r = lax.rem(c + e + 1, 4)

                def act():
                    if flow in DIAG_ROW:
                        rows = pl.ds(DIAG_ROW[flow], BLOCK)
                        part[slot, c, e] = product(panel[r, rows, :], panel[c, rows, :])
                    elif flow in SPLIT_ROW:
                        row, count = SPLIT_ROW[flow]
                        left = panel[r, pl.ds(row, count), :]
                        for b in range(2):
                            part[slot, c, e, pl.ds(first + b * count, count), :] = product(left, panel[c, pl.ds(b * BLOCK, BLOCK), :])
                    else:
                        part[slot, c, e] = product(panel[r, pl.ds(BLOCK, BLOCK), :], panel[c, pl.ds(0, BLOCK), :])

                if_present(flow, c, e, None, act)

            each(tile)

            @pl.when(lax.rem(c, 2) != core)
            def _():
                each(lambda e: if_present(flow, c, e, None, lambda: core_copy(flow, c, e).start()))

            return carry

        lax.fori_loop(0, 4, c_step, 0)

    def core_add(flow):
        def add_in(c, e):
            core_copy(flow, c, e).wait_recv()
            view(part, flow, c, e)[...] += view(core_in, flow, lax.div(c, 2), e)[...]

        def pass_on(e):
            add_in(given, e)
            y_copy(flow, e).start()

        if flow == D2:
            each_d(lambda pair, c, e, r: (add_in(c, e), pl.when(lax.rem(r, 2) != odd)(lambda: d_z1_copy(pair, c, e, r).start())))
            return
        each(lambda e: if_present(flow, given, e, None, lambda: pass_on(e)))
        each(lambda e: if_present(flow, kept, e, None, lambda: add_in(kept, e)))

    def y_add(flow):
        def act(e):
            y_copy(flow, e).wait_recv()
            view(part, flow, kept, e)[...] += view(y_in, flow, e)[...]
            r = lax.rem(kept + e + 1, 4)
            pl.when(lax.rem(r, 2) != odd)(lambda: z1_copy(flow, e, r).start())

        each(lambda e: if_present(flow, kept, e, None, lambda: act(e)))

    def z1_add(flow):
        def act(e, r):
            z1_copy(flow, e, r).wait_recv()
            view(part, flow, kept, e)[...] += view(z1_in, flow, lax.div(r, 2))[...]
            pl.when(r != z)(lambda: z2_copy(flow, e).start())

        def step(e):
            r = lax.rem(kept + e + 1, 4)
            if_present(flow, kept, e, lax.rem(r, 2) == odd, lambda: act(e, r))

        each(step)

    def z2_add(flow):
        def act(e):
            z2_copy(flow, e).wait_recv()
            vals = (view(part, flow, kept, e)[...] + view(z2_in, flow)[...]).astype(out_ref.dtype)
            if flow in DIAG_ROW:
                out_ref[pl.ds(DIAG_ROW[flow], BLOCK), pl.ds(DIAG_ROW[flow], BLOCK)] = vals
            elif flow in SPLIT_ROW:
                row, count = SPLIT_ROW[flow]
                for b in range(2):
                    out_ref[pl.ds(row, count), pl.ds(b * BLOCK, BLOCK)] = vals[b * count:(b + 1) * count]
            else:
                out_ref[pl.ds(BLOCK, BLOCK), pl.ds(0, BLOCK)] = vals

        each(lambda e: if_present(flow, kept, e, lax.rem(kept + e + 1, 4) == z, lambda: act(e)))

    def each_d(act):
        for pair in range(2):
            c = core + 2 * pair
            each(lambda e: pl.when(c + e + 1 < 4)(lambda: (act(pair, c, e, c + e + 1), None)[1]))

    def d_z1_copy(pair, c, e, r):
        half = lax.div(r, 2)
        return remote(part.at[5, c, e], d_z1_in.at[pair, half], d_z1_send.at[pair, half], d_z1_recv.at[pair, half],
                      {'row': peers[0]})

    def d_z2_copy(pair, c, e):
        return remote(part.at[5, c, e], d_z2_in.at[pair], d_z2_send.at[pair], d_z2_recv.at[pair], {'row': peers[1]})

    def d_y_copy(c, e):
        return remote(part.at[5, c, e], y_in.at[5, 0], y_send.at[D2, 0], y_recv.at[D2, 0], y_peer)

    def d_z1_add():
        def act(pair, c, e, r):
            @pl.when(lax.rem(r, 2) == odd)
            def _():
                d_z1_copy(pair, c, e, r).wait_recv()
                part[5, c, e] += d_z1_in[pair, lax.div(r, 2)]
                pl.when(r != z)(lambda: d_z2_copy(pair, c, e).start())

        each_d(act)

    def d_z2_add():
        def act(pair, c, e, r):
            @pl.when(r == z)
            def _():
                d_z2_copy(pair, c, e).wait_recv()
                part[5, c, e] += d_z2_in[pair]
                pl.when(y != pair)(lambda: d_y_copy(c, e).start())

        each_d(act)

    def d_y_add():
        def act(pair, c, e, r):
            @pl.when(jnp.logical_and(r == z, y == pair))
            def _():
                d_y_copy(c, e).wait_recv()
                rows = pl.ds(DIAG_ROW[D2], BLOCK)
                out_ref[rows, rows] = (part[5, c, e] + y_in[5, 0]).astype(out_ref.dtype)

        each_d(act)

    def d_drain():
        def act(pair, c, e, r):
            pl.when(lax.rem(r, 2) != odd)(lambda: d_z1_copy(pair, c, e, r).wait_send())
            pl.when(r == lax.rem(z + 2, 4))(lambda: d_z2_copy(pair, c, e).wait_send())
            pl.when(jnp.logical_and(r == z, y != pair))(lambda: d_y_copy(c, e).wait_send())

        each_d(act)

    def drain(flow):
        for pair in range(2):
            c = 1 - core + 2 * pair
            each(lambda e: if_present(flow, c, e, None, lambda: core_copy(flow, c, e).wait_send()))
        if flow == D2:
            d_drain()
            return
        each(lambda e: if_present(flow, given, e, None, lambda: y_copy(flow, e).wait_send()))

        def step(e):
            r = lax.rem(kept + e + 1, 4)
            if_present(flow, kept, e, lax.rem(r, 2) != odd, lambda: z1_copy(flow, e, r).wait_send())
            if_present(flow, kept, e, r == lax.rem(z + 2, 4), lambda: z2_copy(flow, e).wait_send())

        each(step)

    wait_stage(0)
    compute(D0)
    self_core_add()
    core_add(D0)
    wait_stage(1)
    compute(R1)
    core_add(R1)
    compute(D1)
    core_add(D1)
    self_y_add()
    y_add(D0)
    y_add(R1)
    pl.when(outer)(lambda: start_pairs(every[FIRST_STAGES:], 2, 0))
    y_add(D1)
    wait_stage(2)
    compute(R2A)
    core_add(R2A)
    z1_add(D0)
    z1_add(R1)
    y_add(R2A)
    wait_stage(3)
    compute(R2B)
    core_add(R2B)
    y_add(R2B)
    wait_stage(4)
    compute(D2)
    compute(R2C)
    core_add(D2)
    core_add(R2C)
    z1_add(D1)
    z1_add(R2A)
    z1_add(R2B)
    d_z1_add()
    y_add(R2C)
    z2_add(D0)
    z2_add(R1)
    d_z2_add()
    z1_add(R2C)
    z2_add(D1)
    z2_add(R2A)
    z2_add(R2B)
    d_y_add()
    z2_add(R2C)

    for stage in every:
        pl.when(outer)(lambda: a_copy(stage, 0).wait_send())
        for hop in (1, 2):
            a_copy(stage, hop).wait_send()
    pl.when(jnp.logical_not(right_core))(lambda: self_core.wait_send())
    pl.when(jnp.logical_and(right_core, jnp.logical_not(right_y)))(lambda: self_y.wait_send())
    for flow in range(FLOWS):
        drain(flow)


def solution(mesh):
    def local_fn(a_local):
        local_rows, m_local = a_local.shape
        width = m_local // 4
        deep = min(1024, m_local)
        tile = (BLOCK, BLOCK)
        dma = pltpu.SemaphoreType.DMA
        return pl.pallas_call(
            kernel,
            out_shape=jax.ShapeDtypeStruct((local_rows, local_rows), jnp.bfloat16),
            in_specs=[pl.BlockSpec(memory_space=pl.ANY)],
            out_specs=pl.BlockSpec(memory_space=pltpu.VMEM),
            scratch_shapes=[
                pltpu.VMEM((4, local_rows, width), jnp.bfloat16),
                pltpu.VMEM((2, local_rows, deep), jnp.bfloat16),
                pltpu.VMEM((6,) + tile, jnp.float32),
                pltpu.VMEM((2, 6) + tile, jnp.float32),
                pltpu.VMEM((6, 4, 3) + tile, jnp.float32),
                pltpu.VMEM((6, 2, 3) + tile, jnp.float32),
                pltpu.VMEM((6, 3) + tile, jnp.float32),
                pltpu.VMEM((5, 2) + tile, jnp.float32),
                pltpu.VMEM((5,) + tile, jnp.float32),
                pltpu.VMEM((2, 2) + tile, jnp.float32),
                pltpu.VMEM((2,) + tile, jnp.float32),
                dma((len(STAGES), 3)), dma((len(STAGES), 3)), dma, dma((2,)), dma((2,)), dma((2,)),
                dma((FLOWS, 2, 3)), dma((FLOWS, 2, 3)), dma((FLOWS, 3)), dma((FLOWS, 3)),
                dma((FLOWS, 2)), dma((FLOWS, 2)), dma((FLOWS,)), dma((FLOWS,)),
                dma((2, 2)), dma((2, 2)), dma((2,)), dma((2,)),
            ],
            compiler_params=pltpu.CompilerParams(collective_id=0, has_side_effects=True, vmem_limit_bytes=67043328),
            name='triangle',
        )(a_local)

    part_spec = P(('batch', 'row'), 'col')
    return jax.shard_map(local_fn, mesh=mesh, in_specs=(part_spec,), out_specs=part_spec, check_vma=False)
```

```python
import jax
import jax.numpy as jnp
from jax import lax
from jax.experimental import pallas as pl
from jax.experimental.pallas import tpu as pltpu
from jax.sharding import PartitionSpec as P

BLOCK = 256
MESH = pl.DeviceIdType.MESH
STAGES = ((0, 256), (256, 256), (512, 128), (640, 64), (704, 64))
FIRST_STAGES = 3
FLOWS = 7
D0, R1, D1, R2A, R2B, R2C, D2 = range(FLOWS)
DIAG_ROW = {D0: 0, D1: BLOCK, D2: 2 * BLOCK}
SPLIT_ROW = {R2A: (512, 128), R2B: (640, 64), R2C: (704, 64)}
PLACE = {D0: (0, 0, 256), R1: (1, 0, 256), D1: (2, 0, 256), R2A: (3, 0, 256), R2B: (4, 0, 128), R2C: (4, 128, 128), D2: (5, 0, 256)}
SELF_TILES = ((0, 0), (1, 0), (2, 0), (1, 1), (2, 1), (2, 2))


def product(left, right):
    return lax.dot_general(left, right, (((1,), (1,)), ((), ())), preferred_element_type=jnp.float32)


def kernel(a_ref, out_ref, panel, chunk, own_part, own_recv, part, core_in, y_in, z1_in, z2_in,
           a_send, a_recv, own_sem, chunk_sem, self_send, self_recv,
           core_send, core_recv, y_send, y_recv, z1_send, z1_recv, z2_send, z2_recv):
    z = lax.axis_index('row')
    col = lax.axis_index('col')
    core = lax.rem(col, 2)
    y = lax.div(col, 2)
    odd = lax.rem(z, 2)
    peers = (z + 1 - 2 * odd, lax.rem(z + 2, 4), 3 - z)
    sibling = {'col': col + 1 - 2 * core}
    y_peer = {'col': lax.rem(col + 2, 4)}
    width = panel.shape[2]
    deep = chunk.shape[2]
    kept = col
    given = lax.rem(col + 2, 4)

    barrier = pltpu.get_barrier_semaphore()
    for dev in (sibling, y_peer, {'row': peers[0]}, {'row': peers[1]}, {'row': peers[2]}):
        pl.semaphore_signal(barrier, inc=1, device_id=dev, device_id_type=MESH)
    pl.semaphore_wait(barrier, 5)

    def remote(src, dst, send, recv, dev):
        return pltpu.make_async_remote_copy(src_ref=src, dst_ref=dst, send_sem=send, recv_sem=recv,
                                            device_id=dev, device_id_type=MESH)

    def a_copy(stage, hop):
        first, count = STAGES[stage]
        peer = peers[hop]
        cols = pl.ds(pl.multiple_of(peer * width, 128), width)
        return remote(a_ref.at[pl.ds(first, count), cols], panel.at[z, pl.ds(first, count)],
                      a_send.at[stage, hop], a_recv.at[stage, hop], {'row': peer})

    def start_sends(stages):
        def in_order(order):
            for stage in stages:
                for hop in order:
                    a_copy(stage, hop).start()

        pl.when(core == 0)(lambda: in_order((1, 2, 0)))
        pl.when(core == 1)(lambda: in_order((0, 2, 1)))

    inner = jnp.logical_or(z == 1, z == 2)
    start_sends(range(FIRST_STAGES))
    pl.when(inner)(lambda: start_sends(range(FIRST_STAGES, len(STAGES))))
    own_copy = pltpu.make_async_copy(a_ref.at[:, pl.ds(pl.multiple_of(z * width, 128), width)], panel.at[z], own_sem)
    own_copy.start()

    def chunk_copy(idx, slot):
        cols = pl.ds(pl.multiple_of(idx * deep, 128), deep)
        return pltpu.make_async_copy(a_ref.at[:, cols], chunk.at[slot], chunk_sem.at[slot])

    chunk_copy(0, 0).start()
    out_ref[...] = jnp.zeros_like(out_ref)
    own_part[...] = jnp.zeros_like(own_part)
    chunks = a_ref.shape[1] // deep

    def self_step(idx, carry):
        slot = lax.rem(idx, 2)

        @pl.when(idx + 1 < chunks)
        def _():
            chunk_copy(idx + 1, 1 - slot).start()

        chunk_copy(idx, slot).wait()
        for tile, (up, down) in enumerate(SELF_TILES):
            own_part[tile] += product(chunk[slot, pl.ds(up * BLOCK, BLOCK), :], chunk[slot, pl.ds(down * BLOCK, BLOCK), :])
        return carry

    lax.fori_loop(0, chunks, self_step, 0)
    self_core = remote(own_part, own_recv.at[0], self_send.at[0], self_recv.at[0], sibling)
    self_y = remote(own_part, own_recv.at[1], self_send.at[1], self_recv.at[1], y_peer)
    right_core = core == odd
    right_y = y == lax.div(z, 2)
    pl.when(jnp.logical_not(right_core))(lambda: self_core.start())

    def self_core_add():
        @pl.when(right_core)
        def _():
            self_core.wait_recv()
            own_part[...] += own_recv[0]
            pl.when(jnp.logical_not(right_y))(lambda: self_y.start())

    def self_y_add():
        @pl.when(col == z)
        def _():
            self_y.wait_recv()
            own_part[...] += own_recv[1]
            below = lax.broadcasted_iota(jnp.int32, (BLOCK, BLOCK), 0) >= lax.broadcasted_iota(jnp.int32, (BLOCK, BLOCK), 1)
            for tile, (up, down) in enumerate(SELF_TILES):
                vals = own_part[tile]
                if up == down:
                    vals = jnp.where(below, vals, 0.0)
                out_ref[pl.ds(up * BLOCK, BLOCK), pl.ds(down * BLOCK, BLOCK)] = vals.astype(out_ref.dtype)

    def if_present(flow, c, e, more, act):
        cond = more
        if flow in DIAG_ROW:
            here = c + e + 1 < 4
            cond = here if more is None else jnp.logical_and(more, here)
        if cond is None:
            act()
        else:
            pl.when(cond)(act)

    def view(ref, flow, *idx):
        slot, first, count = PLACE[flow]
        return ref.at[(slot,) + idx + (pl.ds(first, count),)]

    def core_copy(flow, c, e):
        pair = lax.div(c, 2)
        return remote(view(part, flow, c, e), view(core_in, flow, pair, e), core_send.at[flow, pair, e],
                      core_recv.at[flow, pair, e], sibling)

    def y_copy(flow, e):
        return remote(view(part, flow, given, e), view(y_in, flow, e), y_send.at[flow, e], y_recv.at[flow, e], y_peer)

    def z1_copy(flow, e, r):
        pair = lax.div(r, 2)
        return remote(view(part, flow, kept, e), view(z1_in, flow, pair), z1_send.at[flow, pair], z1_recv.at[flow, pair],
                      {'row': peers[0]})

    def z2_copy(flow, e):
        return remote(view(part, flow, kept, e), view(z2_in, flow), z2_send.at[flow], z2_recv.at[flow], {'row': peers[1]})

    def each(act):
        lax.fori_loop(0, 3, lambda e, carry: (act(e), carry)[1], 0)

    def wait_stage(stage):
        if stage == 0:
            own_copy.wait()
        for hop in range(3):
            a_copy(stage, hop).wait_recv()

    def compute(flow):
        slot, first, _ = PLACE[flow]

        def c_step(c, carry):
            def tile(e):
                r = lax.rem(c + e + 1, 4)

                def act():
                    if flow in DIAG_ROW:
                        rows = pl.ds(DIAG_ROW[flow], BLOCK)
                        part[slot, c, e] = product(panel[r, rows, :], panel[c, rows, :])
                    elif flow in SPLIT_ROW:
                        row, count = SPLIT_ROW[flow]
                        left = panel[r, pl.ds(row, count), :]
                        for b in range(2):
                            part[slot, c, e, pl.ds(first + b * count, count), :] = product(left, panel[c, pl.ds(b * BLOCK, BLOCK), :])
                    else:
                        part[slot, c, e] = product(panel[r, pl.ds(BLOCK, BLOCK), :], panel[c, pl.ds(0, BLOCK), :])

                if_present(flow, c, e, None, act)

            each(tile)

            @pl.when(lax.rem(c, 2) != core)
            def _():
                each(lambda e: if_present(flow, c, e, None, lambda: core_copy(flow, c, e).start()))

            return carry

        lax.fori_loop(0, 4, c_step, 0)

    def core_add(flow):
        def add_in(c, e):
            core_copy(flow, c, e).wait_recv()
            view(part, flow, c, e)[...] += view(core_in, flow, lax.div(c, 2), e)[...]

        def pass_on(e):
            add_in(given, e)
            y_copy(flow, e).start()

        each(lambda e: if_present(flow, given, e, None, lambda: pass_on(e)))
        each(lambda e: if_present(flow, kept, e, None, lambda: add_in(kept, e)))

    def y_add(flow):
        def act(e):
            y_copy(flow, e).wait_recv()
            view(part, flow, kept, e)[...] += view(y_in, flow, e)[...]
            r = lax.rem(kept + e + 1, 4)
            pl.when(lax.rem(r, 2) != odd)(lambda: z1_copy(flow, e, r).start())

        each(lambda e: if_present(flow, kept, e, None, lambda: act(e)))

    def z1_add(flow):
        def act(e, r):
            z1_copy(flow, e, r).wait_recv()
            view(part, flow, kept, e)[...] += view(z1_in, flow, lax.div(r, 2))[...]
            pl.when(r != z)(lambda: z2_copy(flow, e).start())

        def step(e):
            r = lax.rem(kept + e + 1, 4)
            if_present(flow, kept, e, lax.rem(r, 2) == odd, lambda: act(e, r))

        each(step)

    def z2_add(flow):
        def act(e):
            z2_copy(flow, e).wait_recv()
            vals = (view(part, flow, kept, e)[...] + view(z2_in, flow)[...]).astype(out_ref.dtype)
            if flow in DIAG_ROW:
                out_ref[pl.ds(DIAG_ROW[flow], BLOCK), pl.ds(DIAG_ROW[flow], BLOCK)] = vals
            elif flow in SPLIT_ROW:
                row, count = SPLIT_ROW[flow]
                for b in range(2):
                    out_ref[pl.ds(row, count), pl.ds(b * BLOCK, BLOCK)] = vals[b * count:(b + 1) * count]
            else:
                out_ref[pl.ds(BLOCK, BLOCK), pl.ds(0, BLOCK)] = vals

        each(lambda e: if_present(flow, kept, e, lax.rem(kept + e + 1, 4) == z, lambda: act(e)))

    def drain(flow):
        for pair in range(2):
            c = 1 - core + 2 * pair
            each(lambda e: if_present(flow, c, e, None, lambda: core_copy(flow, c, e).wait_send()))
        each(lambda e: if_present(flow, given, e, None, lambda: y_copy(flow, e).wait_send()))

        def step(e):
            r = lax.rem(kept + e + 1, 4)
            if_present(flow, kept, e, lax.rem(r, 2) != odd, lambda: z1_copy(flow, e, r).wait_send())
            if_present(flow, kept, e, r == lax.rem(z + 2, 4), lambda: z2_copy(flow, e).wait_send())

        each(step)

    wait_stage(0)
    compute(D0)
    self_core_add()
    core_add(D0)
    wait_stage(1)
    compute(R1)
    core_add(R1)
    compute(D1)
    core_add(D1)
    self_y_add()
    y_add(D0)
    y_add(R1)
    y_add(D1)
    z1_add(D0)
    z1_add(R1)
    pl.when(jnp.logical_not(inner))(lambda: start_sends(range(FIRST_STAGES, len(STAGES))))
    wait_stage(2)
    compute(R2A)
    core_add(R2A)
    y_add(R2A)
    wait_stage(3)
    compute(R2B)
    core_add(R2B)
    y_add(R2B)
    wait_stage(4)
    compute(D2)
    core_add(D2)
    compute(R2C)
    core_add(R2C)
    z1_add(D1)
    z1_add(R2A)
    z1_add(R2B)
    y_add(D2)
    y_add(R2C)
    z1_add(D2)
    z1_add(R2C)
    for flow in (D0, R1, D1, R2A, R2B, D2, R2C):
        z2_add(flow)

    for stage in range(len(STAGES)):
        for hop in range(3):
            a_copy(stage, hop).wait_send()
    pl.when(jnp.logical_not(right_core))(lambda: self_core.wait_send())
    pl.when(jnp.logical_and(right_core, jnp.logical_not(right_y)))(lambda: self_y.wait_send())
    for flow in range(FLOWS):
        drain(flow)


def solution(mesh):
    def local_fn(a_local):
        local_rows, m_local = a_local.shape
        width = m_local // 4
        deep = min(1024, m_local)
        tile = (BLOCK, BLOCK)
        dma = pltpu.SemaphoreType.DMA
        return pl.pallas_call(
            kernel,
            out_shape=jax.ShapeDtypeStruct((local_rows, local_rows), jnp.bfloat16),
            in_specs=[pl.BlockSpec(memory_space=pl.ANY)],
            out_specs=pl.BlockSpec(memory_space=pltpu.VMEM),
            scratch_shapes=[
                pltpu.VMEM((4, local_rows, width), jnp.bfloat16),
                pltpu.VMEM((2, local_rows, deep), jnp.bfloat16),
                pltpu.VMEM((6,) + tile, jnp.float32),
                pltpu.VMEM((2, 6) + tile, jnp.float32),
                pltpu.VMEM((6, 4, 3) + tile, jnp.float32),
                pltpu.VMEM((6, 2, 3) + tile, jnp.float32),
                pltpu.VMEM((6, 3) + tile, jnp.float32),
                pltpu.VMEM((6, 2) + tile, jnp.float32),
                pltpu.VMEM((6,) + tile, jnp.float32),
                dma((len(STAGES), 3)), dma((len(STAGES), 3)), dma, dma((2,)), dma((2,)), dma((2,)),
                dma((FLOWS, 2, 3)), dma((FLOWS, 2, 3)), dma((FLOWS, 3)), dma((FLOWS, 3)),
                dma((FLOWS, 2)), dma((FLOWS, 2)), dma((FLOWS,)), dma((FLOWS,)),
            ],
            compiler_params=pltpu.CompilerParams(collective_id=0, has_side_effects=True, vmem_limit_bytes=67043328),
            name='triangle',
        )(a_local)

    part_spec = P(('batch', 'row'), 'col')
    return jax.shard_map(local_fn, mesh=mesh, in_specs=(part_spec,), out_specs=part_spec, check_vma=False)
```

```python
import jax
import jax.numpy as jnp
from jax import lax
from jax.experimental import pallas as pl
from jax.experimental.pallas import tpu as pltpu
from jax.sharding import PartitionSpec as P

BLOCK = 256
MESH = pl.DeviceIdType.MESH
STAGES = tuple((row, 64) for row in range(0, 3 * BLOCK, 64))
FLOWS = 7
D0, R1, D1, R2A, R2B, R2C, D2 = range(FLOWS)
DIAG_ROW = {D0: 0, D1: BLOCK, D2: 2 * BLOCK}
SPLIT_ROW = {R2A: (512, 128), R2B: (640, 64), R2C: (704, 64)}
PLACE = {D0: (0, 0, 256), R1: (1, 0, 256), D1: (2, 0, 256), R2A: (3, 0, 256), R2B: (4, 0, 128), R2C: (4, 128, 128), D2: (5, 0, 256)}
SELF_TILES = ((0, 0), (1, 0), (2, 0), (1, 1), (2, 1), (2, 2))


def product(left, right):
    return lax.dot_general(left, right, (((1,), (1,)), ((), ())), preferred_element_type=jnp.float32)


def kernel(a_ref, out_ref, panel, chunk, own_part, own_recv, part, core_in, y_in, z1_in, z2_in,
           a_send, a_recv, own_sem, chunk_sem, self_send, self_recv,
           core_send, core_recv, y_send, y_recv, z1_send, z1_recv, z2_send, z2_recv):
    z = lax.axis_index('row')
    col = lax.axis_index('col')
    core = lax.rem(col, 2)
    y = lax.div(col, 2)
    odd = lax.rem(z, 2)
    peers = (z + 1 - 2 * odd, lax.rem(z + 2, 4), 3 - z)
    sibling = {'col': col + 1 - 2 * core}
    y_peer = {'col': lax.rem(col + 2, 4)}
    width = panel.shape[2]
    deep = chunk.shape[2]
    kept = col
    given = lax.rem(col + 2, 4)

    barrier = pltpu.get_barrier_semaphore()
    for dev in (sibling, y_peer, {'row': peers[0]}, {'row': peers[1]}, {'row': peers[2]}):
        pl.semaphore_signal(barrier, inc=1, device_id=dev, device_id_type=MESH)
    pl.semaphore_wait(barrier, 5)

    def remote(src, dst, send, recv, dev):
        return pltpu.make_async_remote_copy(src_ref=src, dst_ref=dst, send_sem=send, recv_sem=recv,
                                            device_id=dev, device_id_type=MESH)

    def a_copy(stage, hop):
        first, count = STAGES[stage]
        peer = peers[hop]
        cols = pl.ds(pl.multiple_of(peer * width, 128), width)
        return remote(a_ref.at[pl.ds(first, count), cols], panel.at[z, pl.ds(first, count)],
                      a_send.at[stage, hop], a_recv.at[stage, hop], {'row': peer})

    def start_sends(stages):
        def in_order(order):
            for stage in stages:
                for hop in order:
                    a_copy(stage, hop).start()

        pl.when(core == 0)(lambda: in_order((1, 2, 0)))
        pl.when(core == 1)(lambda: in_order((0, 2, 1)))

    start_sends((0, 1))
    own_copy = pltpu.make_async_copy(a_ref.at[:, pl.ds(pl.multiple_of(z * width, 128), width)], panel.at[z], own_sem)
    own_copy.start()

    def chunk_copy(idx, slot):
        cols = pl.ds(pl.multiple_of(idx * deep, 128), deep)
        return pltpu.make_async_copy(a_ref.at[:, cols], chunk.at[slot], chunk_sem.at[slot])

    chunk_copy(0, 0).start()
    out_ref[...] = jnp.zeros_like(out_ref)
    own_part[...] = jnp.zeros_like(own_part)
    chunks = a_ref.shape[1] // deep

    def self_step(idx, carry):
        slot = lax.rem(idx, 2)

        @pl.when(idx + 1 < chunks)
        def _():
            chunk_copy(idx + 1, 1 - slot).start()

        chunk_copy(idx, slot).wait()
        for tile, (up, down) in enumerate(SELF_TILES):
            own_part[tile] += product(chunk[slot, pl.ds(up * BLOCK, BLOCK), :], chunk[slot, pl.ds(down * BLOCK, BLOCK), :])
        return carry

    lax.fori_loop(0, chunks, self_step, 0)
    self_core = remote(own_part, own_recv.at[0], self_send.at[0], self_recv.at[0], sibling)
    self_y = remote(own_part, own_recv.at[1], self_send.at[1], self_recv.at[1], y_peer)
    right_core = core == odd
    right_y = y == lax.div(z, 2)
    pl.when(jnp.logical_not(right_core))(lambda: self_core.start())

    def self_core_add():
        @pl.when(right_core)
        def _():
            self_core.wait_recv()
            own_part[...] += own_recv[0]
            pl.when(jnp.logical_not(right_y))(lambda: self_y.start())

    def self_y_add():
        @pl.when(col == z)
        def _():
            self_y.wait_recv()
            own_part[...] += own_recv[1]
            below = lax.broadcasted_iota(jnp.int32, (BLOCK, BLOCK), 0) >= lax.broadcasted_iota(jnp.int32, (BLOCK, BLOCK), 1)
            for tile, (up, down) in enumerate(SELF_TILES):
                vals = own_part[tile]
                if up == down:
                    vals = jnp.where(below, vals, 0.0)
                out_ref[pl.ds(up * BLOCK, BLOCK), pl.ds(down * BLOCK, BLOCK)] = vals.astype(out_ref.dtype)

    def if_present(flow, c, e, more, act):
        cond = more
        if flow in DIAG_ROW:
            here = c + e + 1 < 4
            cond = here if more is None else jnp.logical_and(more, here)
        if cond is None:
            act()
        else:
            pl.when(cond)(act)

    def view(ref, flow, *idx):
        slot, first, count = PLACE[flow]
        return ref.at[(slot,) + idx + (pl.ds(first, count),)]

    def core_copy(flow, c, e):
        pair = lax.div(c, 2)
        return remote(view(part, flow, c, e), view(core_in, flow, pair, e), core_send.at[flow, pair, e],
                      core_recv.at[flow, pair, e], sibling)

    def y_copy(flow, e):
        return remote(view(part, flow, given, e), view(y_in, flow, e), y_send.at[flow, e], y_recv.at[flow, e], y_peer)

    def z1_copy(flow, e, r):
        pair = lax.div(r, 2)
        return remote(view(part, flow, kept, e), view(z1_in, flow, pair), z1_send.at[flow, pair], z1_recv.at[flow, pair],
                      {'row': peers[0]})

    def z2_copy(flow, e):
        return remote(view(part, flow, kept, e), view(z2_in, flow), z2_send.at[flow], z2_recv.at[flow], {'row': peers[1]})

    def each(act):
        lax.fori_loop(0, 3, lambda e, carry: (act(e), carry)[1], 0)

    def wait_stage(stage):
        if stage == 0:
            own_copy.wait()
        for hop in range(3):
            a_copy(stage, hop).wait_recv()

    def compute(flow):
        slot, first, _ = PLACE[flow]

        def c_step(c, carry):
            def tile(e):
                r = lax.rem(c + e + 1, 4)

                def act():
                    if flow in DIAG_ROW:
                        rows = pl.ds(DIAG_ROW[flow], BLOCK)
                        part[slot, c, e] = product(panel[r, rows, :], panel[c, rows, :])
                    elif flow in SPLIT_ROW:
                        row, count = SPLIT_ROW[flow]
                        left = panel[r, pl.ds(row, count), :]
                        for b in range(2):
                            part[slot, c, e, pl.ds(first + b * count, count), :] = product(left, panel[c, pl.ds(b * BLOCK, BLOCK), :])
                    else:
                        part[slot, c, e] = product(panel[r, pl.ds(BLOCK, BLOCK), :], panel[c, pl.ds(0, BLOCK), :])

                if_present(flow, c, e, None, act)

            each(tile)

            @pl.when(lax.rem(c, 2) != core)
            def _():
                each(lambda e: if_present(flow, c, e, None, lambda: core_copy(flow, c, e).start()))

            return carry

        lax.fori_loop(0, 4, c_step, 0)

    def core_add(flow):
        def add_in(c, e):
            core_copy(flow, c, e).wait_recv()
            view(part, flow, c, e)[...] += view(core_in, flow, lax.div(c, 2), e)[...]

        def pass_on(e):
            add_in(given, e)
            y_copy(flow, e).start()

        each(lambda e: if_present(flow, given, e, None, lambda: pass_on(e)))
        each(lambda e: if_present(flow, kept, e, None, lambda: add_in(kept, e)))

    def y_add(flow):
        def act(e):
            y_copy(flow, e).wait_recv()
            view(part, flow, kept, e)[...] += view(y_in, flow, e)[...]
            r = lax.rem(kept + e + 1, 4)
            pl.when(lax.rem(r, 2) != odd)(lambda: z1_copy(flow, e, r).start())

        each(lambda e: if_present(flow, kept, e, None, lambda: act(e)))

    def z1_add(flow):
        def act(e, r):
            z1_copy(flow, e, r).wait_recv()
            view(part, flow, kept, e)[...] += view(z1_in, flow, lax.div(r, 2))[...]
            pl.when(r != z)(lambda: z2_copy(flow, e).start())

        def step(e):
            r = lax.rem(kept + e + 1, 4)
            if_present(flow, kept, e, lax.rem(r, 2) == odd, lambda: act(e, r))

        each(step)

    def z2_add(flow):
        def act(e):
            z2_copy(flow, e).wait_recv()
            vals = (view(part, flow, kept, e)[...] + view(z2_in, flow)[...]).astype(out_ref.dtype)
            if flow in DIAG_ROW:
                out_ref[pl.ds(DIAG_ROW[flow], BLOCK), pl.ds(DIAG_ROW[flow], BLOCK)] = vals
            elif flow in SPLIT_ROW:
                row, count = SPLIT_ROW[flow]
                for b in range(2):
                    out_ref[pl.ds(row, count), pl.ds(b * BLOCK, BLOCK)] = vals[b * count:(b + 1) * count]
            else:
                out_ref[pl.ds(BLOCK, BLOCK), pl.ds(0, BLOCK)] = vals

        each(lambda e: if_present(flow, kept, e, lax.rem(kept + e + 1, 4) == z, lambda: act(e)))

    def drain(flow):
        for pair in range(2):
            c = 1 - core + 2 * pair
            each(lambda e: if_present(flow, c, e, None, lambda: core_copy(flow, c, e).wait_send()))
        each(lambda e: if_present(flow, given, e, None, lambda: y_copy(flow, e).wait_send()))

        def step(e):
            r = lax.rem(kept + e + 1, 4)
            if_present(flow, kept, e, lax.rem(r, 2) != odd, lambda: z1_copy(flow, e, r).wait_send())
            if_present(flow, kept, e, r == lax.rem(z + 2, 4), lambda: z2_copy(flow, e).wait_send())

        each(step)

    wait_stage(0)
    start_sends((2,))
    self_core_add()
    wait_stage(1)
    start_sends((3,))
    wait_stage(2)
    start_sends((4,))
    wait_stage(3)
    compute(D0)
    core_add(D0)
    start_sends((5,))
    wait_stage(4)
    start_sends((6,))
    self_y_add()
    wait_stage(5)
    start_sends((7,))
    wait_stage(6)
    start_sends((8,))
    y_add(D0)
    wait_stage(7)
    compute(R1)
    core_add(R1)
    compute(D1)
    core_add(D1)
    start_sends((9,))
    wait_stage(8)
    start_sends((10,))
    z1_add(D0)
    wait_stage(9)
    compute(R2A)
    core_add(R2A)
    y_add(R1)
    start_sends((11,))
    y_add(D1)
    wait_stage(10)
    compute(R2B)
    core_add(R2B)
    z1_add(R1)
    y_add(R2A)
    wait_stage(11)
    compute(D2)
    core_add(D2)
    compute(R2C)
    core_add(R2C)
    z1_add(D1)
    z1_add(R2A)
    y_add(R2B)
    y_add(D2)
    y_add(R2C)
    z1_add(R2B)
    z1_add(D2)
    z1_add(R2C)
    for flow in (D0, R1, D1, R2A, R2B, D2, R2C):
        z2_add(flow)

    for stage in range(len(STAGES)):
        for hop in range(3):
            a_copy(stage, hop).wait_send()
    pl.when(jnp.logical_not(right_core))(lambda: self_core.wait_send())
    pl.when(jnp.logical_and(right_core, jnp.logical_not(right_y)))(lambda: self_y.wait_send())
    for flow in range(FLOWS):
        drain(flow)


def solution(mesh):
    def local_fn(a_local):
        local_rows, m_local = a_local.shape
        width = m_local // 4
        deep = min(1024, m_local)
        tile = (BLOCK, BLOCK)
        dma = pltpu.SemaphoreType.DMA
        return pl.pallas_call(
            kernel,
            out_shape=jax.ShapeDtypeStruct((local_rows, local_rows), jnp.bfloat16),
            in_specs=[pl.BlockSpec(memory_space=pl.ANY)],
            out_specs=pl.BlockSpec(memory_space=pltpu.VMEM),
            scratch_shapes=[
                pltpu.VMEM((4, local_rows, width), jnp.bfloat16),
                pltpu.VMEM((2, local_rows, deep), jnp.bfloat16),
                pltpu.VMEM((6,) + tile, jnp.float32),
                pltpu.VMEM((2, 6) + tile, jnp.float32),
                pltpu.VMEM((6, 4, 3) + tile, jnp.float32),
                pltpu.VMEM((6, 2, 3) + tile, jnp.float32),
                pltpu.VMEM((6, 3) + tile, jnp.float32),
                pltpu.VMEM((6, 2) + tile, jnp.float32),
                pltpu.VMEM((6,) + tile, jnp.float32),
                dma((len(STAGES), 3)), dma((len(STAGES), 3)), dma, dma((2,)), dma((2,)), dma((2,)),
                dma((FLOWS, 2, 3)), dma((FLOWS, 2, 3)), dma((FLOWS, 3)), dma((FLOWS, 3)),
                dma((FLOWS, 2)), dma((FLOWS, 2)), dma((FLOWS,)), dma((FLOWS,)),
            ],
            compiler_params=pltpu.CompilerParams(collective_id=0, has_side_effects=True, vmem_limit_bytes=67043328),
            name='triangle',
        )(a_local)

    part_spec = P(('batch', 'row'), 'col')
    return jax.shard_map(local_fn, mesh=mesh, in_specs=(part_spec,), out_specs=part_spec, check_vma=False)
```
